256 devices in a mesh: grp: 2 (over z_hi), dev: 128 (over x, z_lo, y, core).
Axes of the slice: x: 4, y: 4, z: 8 (z_hi: 2, z_lo: 4; z = z_hi * 4 + z_lo), core: 2. Of those that a mesh axis runs over, the one named last changes fastest.
Arguments:
- voltages: int32 [512, 137216], P('dev', 'grp'), may hold values from -2147483648 to 2147483646
- block_order: int32 [10], replicated, may hold values from 0 to 9, each once
Outputs:
- visibilities: float32 [10, 2, 2, 1024, 128, 128], P('grp', None, None, 'dev')
The draws below stay inside these ranges and needn't reach their ends.
Inputs may be any that keep to these rules, and one draw needn't show every extreme that they name: `block_order`: a permutation of the block pair numbers.
All inputs are finite; a program needn't handle non-finite values.
Results may differ from the reference program's by a relative error of at most 0.0058.
Values may be sent and summed in bfloat16 or wider, within the bound.
A program may use at most 128 MiB of HBM per device.

```python
import jax
import jax.numpy as jnp
import numpy as np
from jax import lax

A = 512
FREQ_CHANNELS = 1024
FILTER_TAPS = 4
BLOCK_FRAMES = 64
INTEG_PERIODS = 2
BLOCK = 128
NBP = 10
SBLK = 137216
N_GRP = 2


def touch_ends(drawn, stream_key, smallest, high):
    longest = drawn.shape.index(max(drawn.shape))
    spots = []
    for shift in (0, 1):
        where = [jax.random.randint(jax.random.fold_in(stream_key, axis), (), 0, length) for axis, length in enumerate(drawn.shape)]
        where[longest] = (where[longest] + shift) % drawn.shape[longest]
        spots.append(tuple(where))
    return drawn.at[spots[0]].set(smallest).at[spots[1]].set(high)


def setup_inputs(seed: int = 0) -> dict:
    arg_keys = jax.random.split(jax.random.key(seed), 3)
    return {
        "voltages": touch_ends(jax.random.randint(arg_keys[0], (A, N_GRP * INTEG_PERIODS * SBLK // 4), -2147483648, 2147483647), jax.random.fold_in(arg_keys[0], 1), -2147483648, 2147483646).astype(jnp.int32),
        "block_order": jax.random.permutation(arg_keys[1], NBP).astype(jnp.int32),
    }


def unpack_packed_words(words):
    pieces = []
    for byte in range(4):
        raw = jnp.bitwise_and(jnp.right_shift(words, 8 * byte), 255)
        pieces.append((raw - 128).astype(jnp.float32) / 64.0)
    return jnp.concatenate(pieces, axis=-1)


def prototype():
    length = 2 * FREQ_CHANNELS
    position = jnp.arange(FILTER_TAPS * length, dtype=jnp.float32) + 0.5
    window = 0.5 - 0.5 * jnp.cos(2.0 * jnp.pi * position / (length * FILTER_TAPS))
    return jnp.sinc(position / length - FILTER_TAPS / 2.0) * window


def dft_table():
    length = 2 * FREQ_CHANNELS
    index = jnp.arange(length, dtype=jnp.int32)[:, None] * jnp.arange(FREQ_CHANNELS, dtype=jnp.int32)[None, :]
    angle = (2.0 * jnp.pi / length) * (index % length).astype(jnp.float32)
    factor = length ** -0.5
    return jnp.stack([jnp.cos(angle) * factor, -jnp.sin(angle) * factor], axis=1).astype(jnp.bfloat16)


def filter_frames(voltage_samples, coeffs):
    weights = coeffs.reshape(FILTER_TAPS, 2 * FREQ_CHANNELS)
    total = voltage_samples[..., 0:BLOCK_FRAMES, :] * weights[0]
    for shift in range(1, FILTER_TAPS):
        total = total + voltage_samples[..., shift:shift + BLOCK_FRAMES, :] * weights[shift]
    return total.astype(jnp.bfloat16)


def pick(table, index):
    hits = jnp.arange(table.shape[0], dtype=jnp.int32) == index
    return jnp.sum(jnp.where(hits, table, 0)).astype(jnp.int32)


def block_gram(data, slots, block_order, factor):
    twisted = jnp.stack([data[..., 1, :], -data[..., 0, :]], axis=-2)
    upper_rows, upper_cols = np.triu_indices(A // BLOCK)
    pair_rows = jnp.asarray(upper_rows.astype(np.int32))
    pair_cols = jnp.asarray(upper_cols.astype(np.int32))

    def one_slot(slot):
        entry = pick(block_order, slot)
        row = pick(pair_rows, entry) * BLOCK
        col = pick(pair_cols, entry) * BLOCK
        left = lax.dynamic_slice_in_dim(data, row, BLOCK, 1).astype(jnp.float32)
        left_twist = lax.dynamic_slice_in_dim(twisted, row, BLOCK, 1).astype(jnp.float32)
        right = lax.dynamic_slice_in_dim(data, col, BLOCK, 1).astype(jnp.float32)
        real = jnp.einsum('cagirf,cbgirf->icab', left, right)
        imag = jnp.einsum('cagirf,cbgirf->icab', left_twist, right)
        return jnp.stack([real, imag], axis=1) * factor

    return lax.map(one_slot, slots)


def reference(voltages, block_order):
    coeffs = prototype()
    table = dft_table().astype(jnp.float32)
    words = voltages.reshape(A, N_GRP, INTEG_PERIODS, -1)
    groups = []
    for group in range(N_GRP):
        integrations = []
        for integ in range(INTEG_PERIODS):
            voltage_samples = unpack_packed_words(words[:, group, integ]).reshape(A, BLOCK_FRAMES + FILTER_TAPS - 1, 2 * FREQ_CHANNELS)
            filtered = filter_frames(voltage_samples, coeffs)
            channel_spectra = jnp.einsum('afn,nrc->carf', filtered.astype(jnp.float32), table)
            integrations.append(channel_spectra.astype(jnp.bfloat16))
        groups.append(jnp.stack(integrations, axis=2))
    data = jnp.stack(groups, axis=2)
    slots = jnp.arange(NBP, dtype=jnp.int32)
    return block_gram(data, slots, block_order, 1.0 / (N_GRP * BLOCK_FRAMES))
```

```python
import jax
import jax.numpy as jnp
import ml_dtypes
import numpy as np
from jax import lax
from jax.experimental import pallas as pl
from jax.experimental.pallas import tpu as pltpu
from jax.sharding import PartitionSpec as P

MESH = pl.DeviceIdType.MESH
BF16 = jnp.bfloat16
F32 = jnp.float32

A = 512
C = 1024
N = 2 * C
TAPS = 4
F = 64
I = 2
G = 2
LANES = 128
NB = N // LANES
LOCAL = 4
CH = 8
X = Z = Y = 4
K = 2
PLANE = X * Y * K
PIECE = CH * LOCAL
WORDS = 34304
TILES = WORDS // LANES
SLOTS = 5


def prototype():
    position = np.arange(TAPS * N) + 0.5
    window = 0.5 - 0.5 * np.cos(2.0 * np.pi * position / (N * TAPS))
    coeffs = (np.sinc(position / N - TAPS / 2.0) * window).astype(np.float32) / 64
    return coeffs.reshape(TAPS, NB, LANES).transpose(1, 0, 2).reshape(NB * TAPS, LANES)


def dft_table():
    index = (np.arange(C)[:, None] * np.arange(N)[None, :]) % N
    angle = 2.0 * np.pi / N * np.arange(N)
    factor = N**-0.5
    parts = np.stack([np.cos(angle) * factor, -np.sin(angle) * factor])
    parts = parts.astype(np.float32).astype(ml_dtypes.bfloat16)[:, index]
    parts = parts.reshape(2, X, Z, C // (X * Z), N).transpose(2, 0, 1, 3, 4)
    return np.ascontiguousarray(parts.reshape(Z, 2 * C // Z, N))


def front_kernel(v_hbm, coef, tab_hbm, s_hbm, v, x, fs, fb, tab, sf, s, sems):
    load = pltpu.make_async_copy(v_hbm, v, sems.at[0])
    load.start()
    tables = [pltpu.make_async_copy(tab_hbm.at[t], tab.at[t], sems.at[1 + t]) for t in range(Z)]
    load.wait()
    for table in tables:
        table.start()

    def unpack(tile, carry):
        at = pl.multiple_of(tile * LANES, LANES)
        words = jnp.concatenate([v[:, pl.ds(at, LANES)], v[:, pl.ds(at + WORDS, LANES)]], axis=0)
        for byte in range(4):
            raw = jnp.bitwise_and(jnp.right_shift(words, 8 * byte), 255) - 128
            x[byte * TILES + tile] = raw.astype(F32)
        return carry

    lax.fori_loop(0, TILES, unpack, 0, unroll=4)

    def fir(nb, carry):
        c = [coef[pl.ds(nb * TAPS + k, 1), :] for k in range(TAPS)]
        window = [x[k * NB + nb] for k in range(TAPS - 1)]
        for f in range(F):
            window.append(x[(f + TAPS - 1) * NB + nb])
            total = window[0] * c[0]
            for k in range(1, TAPS):
                total = total + window[k] * c[k]
            window.pop(0)
            fs[pl.ds(f, 8, stride=F), :] = total
        fb[:, pl.ds(pl.multiple_of(nb * LANES, LANES), LANES)] = fs[...].astype(BF16)
        return carry

    lax.fori_loop(0, NB, fir, 0)

    low = lax.broadcasted_iota(jnp.int32, (C // Z, LANES), 1) < F
    rows = C // Z
    outs = []
    for t in range(Z):
        tables[t].wait()
        spectra = lax.dot_general(
            tab[t], fb[...], (((1,), (1,)), ((), ())), preferred_element_type=F32
        )
        for i in range(I):
            for pair in range(LOCAL // 2):
                tile = (i * LOCAL // 2 + pair) * LANES
                re = spectra[:rows, tile : tile + LANES]
                im = spectra[rows:, tile : tile + LANES]
                even = jnp.where(low, re, pltpu.roll(im, F, 1))
                odd = jnp.where(low, pltpu.roll(re, F, 1), im)
                sf[i, pl.ds(2 * pair, rows, stride=LOCAL), :] = even
                sf[i, pl.ds(2 * pair + 1, rows, stride=LOCAL), :] = odd
            s[t, :, i] = sf[i].reshape(PLANE, PIECE, LANES).astype(BF16)
        out = pltpu.make_async_copy(s.at[t], s_hbm.at[t], sems.at[1 + Z + t])
        out.start()
        outs.append(out)
    for out in outs:
        out.wait()


def front(voltages):
    coef = jnp.asarray(prototype())
    table = jnp.asarray(dft_table())
    return pl.pallas_call(
        front_kernel,
        name="front",
        out_shape=jax.ShapeDtypeStruct((Z, PLANE, I, PIECE, LANES), BF16),
        in_specs=[
            pl.BlockSpec(memory_space=pl.ANY),
            pl.BlockSpec(memory_space=pltpu.VMEM),
            pl.BlockSpec(memory_space=pl.ANY),
        ],
        out_specs=pl.BlockSpec(memory_space=pl.ANY),
        scratch_shapes=[
            pltpu.VMEM((LOCAL, I * WORDS), jnp.int32),
            pltpu.VMEM((4 * TILES, I * LOCAL, LANES), F32),
            pltpu.VMEM((I * LOCAL * F, LANES), F32),
            pltpu.VMEM((I * LOCAL * F, N), BF16),
            pltpu.VMEM((Z, 2 * C // Z, N), BF16),
            pltpu.VMEM((I, C // Z * LOCAL, LANES), F32),
            pltpu.VMEM((Z, PLANE, I, PIECE, LANES), BF16),
            pltpu.SemaphoreType.DMA((1 + 2 * Z,)),
        ],
        compiler_params=pltpu.CompilerParams(vmem_limit_bytes=48 * 1024 * 1024),
    )(voltages, coef, table)


ORDER = (0, 2, 1, 3)


def turn_kernel(s, r, b, c, hop, plane_send, plane_recv, own_sem, send, recv, hop_send, hop_recv, far_send, far_recv):
    grp = lax.axis_index("grp")
    dev = lax.axis_index("dev")
    x, z, y, k = dev // 32, (dev // 8) % 4, (dev // 2) % 4, dev % 2

    def at_plane(n):
        place = (x * 8 + y * 2 + k) ^ n
        return place, (grp, (place // 8) * 32 + z * 8 + place % 8)

    def at_ring(height):
        height = lax.rem(height + 2 * Z, 2 * Z)
        return (height // Z, x * 32 + (height % Z) * 8 + y * 2 + k)

    here = grp * Z + z
    mine = x * 8 + y * 2 + k

    barrier = pltpu.get_barrier_semaphore()

    def greet_plane(n, carry):
        _, device = at_plane(n)
        pl.semaphore_signal(barrier, inc=1, device_id=device, device_id_type=MESH)
        return carry

    def greet_ring(n, carry):
        pl.semaphore_signal(barrier, inc=1, device_id=at_ring(here + n), device_id_type=MESH)
        return carry

    lax.fori_loop(1, PLANE, greet_plane, 0)
    lax.fori_loop(1, G * Z, greet_ring, 0)
    pl.semaphore_wait(barrier, PLANE + G * Z - 2)

    def target(step):
        return lax.rem(z + step, Z)

    own = []
    for j, step in enumerate(ORDER):
        t = target(step)

        def spread(n, carry):
            place, device = at_plane(n)
            pltpu.make_async_remote_copy(
                s.at[t, place], b.at[j, mine], plane_send.at[j], plane_recv.at[j], device, MESH
            ).start()
            return carry

        lax.fori_loop(1, PLANE, spread, 0)
        copy = pltpu.make_async_copy(s.at[t, mine], b.at[j, mine], own_sem.at[j])
        copy.start()
        own.append(copy)

    row = lax.broadcasted_iota(jnp.int32, (256, 256), 0)
    col = lax.broadcasted_iota(jnp.int32, (256, 256), 1)
    source = ((row >> 2) & 7) * 32 + (row >> 5) * 4 + (row & 3)
    order = (source == col).astype(F32).astype(BF16)

    sends = []
    half = CH * X
    for j, step in enumerate(ORDER):
        own[j].wait()
        whole = pl.ds(0, PLANE - 1)
        pltpu.make_async_copy(b.at[j, whole], b.at[j, whole], plane_recv.at[j]).wait()
        for xs in range(X):
            pieces = [b[j, xs * 8 : xs * 8 + 8, i].reshape(256, LANES) for i in range(I)]
            mixed = jnp.dot(order, jnp.concatenate(pieces, axis=1), preferred_element_type=F32)
            for i in range(I):
                part = mixed[:, i * LANES : (i + 1) * LANES].astype(BF16)
                c[j, i, :, xs] = part.reshape(CH, PIECE, LANES)
        if step == 0:
            copy = pltpu.make_async_copy(c.at[j], r.at[grp, :, :, :, z], own_sem.at[j])
            copy.start()
            local = copy
            for i, way in enumerate((1, -1)):
                copy = pltpu.make_async_remote_copy(
                    c.at[j, i], hop.at[i], hop_send.at[i], hop_recv.at[i], at_ring(here + way), MESH
                )
                copy.start()
                sends.append(copy)
        else:
            for other in range(G):
                to = lax.rem(grp + other, G)
                copy = pltpu.make_async_remote_copy(
                    c.at[j],
                    r.at[grp, :, :, :, z],
                    send.at[j, other],
                    recv.at[j, other],
                    at_ring(to * Z + target(step)),
                    MESH,
                )
                copy.start()
                sends.append(copy)
        if j == 1:
            for i, way in enumerate((1, -1)):
                sends[i].wait_recv()
                origin = lax.rem(here - way + G * Z, G * Z)
                copy = pltpu.make_async_remote_copy(
                    hop.at[i],
                    r.at[origin // Z, i, :, :, origin % Z],
                    far_send.at[i],
                    far_recv.at[i],
                    at_ring(here + 3 * way),
                    MESH,
                )
                copy.start()
                sends.append(copy)
    local.wait()
    for copy in sends[:2]:
        copy.wait_send()
    for copy in sends[2:]:
        copy.wait()
    for j in range(Z):
        whole = pl.ds(0, PLANE - 1)
        pltpu.make_async_copy(s.at[0, whole], s.at[0, whole], plane_send.at[j]).wait()


def turn(spectra):
    return pl.pallas_call(
        turn_kernel,
        name="turn",
        out_shape=jax.ShapeDtypeStruct((G, I, CH, X, Z, PIECE, LANES), BF16),
        in_specs=[pl.BlockSpec(memory_space=pl.ANY)],
        out_specs=pl.BlockSpec(memory_space=pl.ANY),
        scratch_shapes=[
            pltpu.VMEM((Z, PLANE, I, PIECE, LANES), BF16),
            pltpu.VMEM((Z, I, CH, X, PIECE, LANES), BF16),
            pltpu.VMEM((I, CH, X, PIECE, LANES), BF16),
            pltpu.SemaphoreType.DMA((Z,)),
            pltpu.SemaphoreType.DMA((Z,)),
            pltpu.SemaphoreType.DMA((Z,)),
            pltpu.SemaphoreType.DMA((Z, G)),
            pltpu.SemaphoreType.DMA((Z, G)),
            pltpu.SemaphoreType.DMA((2,)),
            pltpu.SemaphoreType.DMA((2,)),
            pltpu.SemaphoreType.DMA((2,)),
            pltpu.SemaphoreType.DMA((2,)),
        ],
        compiler_params=pltpu.CompilerParams(
            collective_id=0, has_side_effects=True, vmem_limit_bytes=48 * 1024 * 1024
        ),
    )(spectra)


def gram_kernel(order, r_hbm, out, r, sems):
    i, s = pl.program_id(0), pl.program_id(1)
    loads = [pltpu.make_async_copy(r_hbm.at[:, n], r.at[n], sems.at[n]) for n in range(I)]

    @pl.when((i == 0) & (s == 0))
    def _():
        for load in loads:
            load.start()

    for n in range(I):

        @pl.when((i == n) & (s == 0))
        def _(n=n):
            loads[n].wait()

    entry = order[lax.axis_index("grp") * SLOTS + s]
    one = lambda bound: (entry >= bound).astype(jnp.int32)
    p = one(4) + one(7) + one(9)
    q = entry - (3 * one(4) + 2 * one(7) + one(9))

    for ch in range(CH):
        left, twisted, right = [], [], []
        for g in range(G):
            block = r[i, g, ch, p]
            wide = block.astype(F32)
            left.append(block)
            twisted.append(jnp.concatenate([wide[:, F:], -wide[:, :F]], axis=1).astype(BF16))
            right.append(r[i, g, ch, q])
        both = jnp.concatenate(
            [jnp.concatenate(left, axis=1), jnp.concatenate(twisted, axis=1)], axis=0
        )
        sums = lax.dot_general(
            both,
            jnp.concatenate(right, axis=1),
            (((1,), (1,)), ((), ())),
            preferred_element_type=F32,
        )
        sums = sums * (1.0 / (G * F))
        out[0, 0, 0, ch] = sums[:LANES]
        out[0, 0, 1, ch] = sums[LANES:]


def gram(block_order, data):
    return pl.pallas_call(
        gram_kernel,
        name="gram",
        out_shape=jax.ShapeDtypeStruct((SLOTS, I, 2, CH, LANES, LANES), F32),
        grid_spec=pltpu.PrefetchScalarGridSpec(
            num_scalar_prefetch=1,
            grid=(I, SLOTS),
            in_specs=[pl.BlockSpec(memory_space=pl.ANY)],
            out_specs=pl.BlockSpec(
                (1, 1, 2, CH, LANES, LANES), lambda i, s, order: (s, i, 0, 0, 0, 0)
            ),
            scratch_shapes=[
                pltpu.VMEM((I, G, CH, X, LANES, LANES), BF16),
                pltpu.SemaphoreType.DMA((I,)),
            ],
        ),
        compiler_params=pltpu.CompilerParams(vmem_limit_bytes=48 * 1024 * 1024),
    )(block_order, data)


def on_device(voltages, block_order):
    spectra = front(voltages)
    data = turn(spectra)
    return gram(block_order, data.reshape(G, I, CH, X, LANES, LANES))


def solution(mesh):
    in_specs = (P("dev", "grp"), P())
    out_specs = P("grp", None, None, "dev", None, None)
    return jax.shard_map(
        on_device, mesh=mesh, in_specs=in_specs, out_specs=out_specs, check_vma=False
    )
```

```python
import jax
import jax.numpy as jnp
import ml_dtypes
import numpy as np
from jax import lax
from jax.experimental import pallas as pl
from jax.experimental.pallas import tpu as pltpu
from jax.sharding import PartitionSpec as P

MESH = pl.DeviceIdType.MESH
BF16 = jnp.bfloat16
F32 = jnp.float32

A = 512
C = 1024
N = 2 * C
TAPS = 4
F = 64
I = 2
G = 2
LANES = 128
NB = N // LANES
LOCAL = 4
CH = 8
X = Z = Y = 4
PLANE = X * Y * 2
H = 2
HC = CH // H
PIECE = HC * LOCAL
ROWS = 8 * LOCAL
UNITS = H * Z
STEP = F + 8
SPLIT = 2
WORDS = 34304
TILES = WORDS // LANES
SLOTS = 5


def prototype():
    position = np.arange(TAPS * N) + 0.5
    window = 0.5 - 0.5 * np.cos(2.0 * np.pi * position / (N * TAPS))
    coeffs = (np.sinc(position / N - TAPS / 2.0) * window).astype(np.float32) / 64
    return coeffs.reshape(TAPS, NB, LANES).transpose(1, 0, 2).reshape(NB * TAPS, LANES)


def dft_table():
    index = (np.arange(C)[:, None] * np.arange(N)[None, :]) % N
    angle = 2.0 * np.pi / N * np.arange(N)
    factor = N**-0.5
    parts = np.stack([np.cos(angle) * factor, -np.sin(angle) * factor])
    parts = parts.astype(np.float32).astype(ml_dtypes.bfloat16)[:, index]
    parts = parts.reshape(2, X, Z, 8, H, HC, N).transpose(2, 4, 0, 1, 3, 5, 6)
    return np.ascontiguousarray(parts.reshape(Z, H, 2 * C // UNITS, N))


def correlate(order, slot, block, store):
    entry = order[slot]
    one = lambda bound: (entry >= bound).astype(jnp.int32)
    p = one(4) + one(7) + one(9)
    q = entry - (3 * one(4) + 2 * one(7) + one(9))
    for i in range(I):
        for ch in range(HC):
            left, twisted, right = [], [], []
            for g in range(G):
                data = block(g, i, ch, p)
                wide = data.astype(F32)
                left.append(data)
                twisted.append(jnp.concatenate([wide[:, F:], -wide[:, :F]], axis=1).astype(BF16))
                right.append(block(g, i, ch, q))
            both = jnp.concatenate(
                [jnp.concatenate(left, axis=1), jnp.concatenate(twisted, axis=1)], axis=0
            )
            sums = lax.dot_general(
                both,
                jnp.concatenate(right, axis=1),
                (((1,), (1,)), ((), ())),
                preferred_element_type=F32,
            )
            sums = sums * (1.0 / (G * F))
            store(i, ch, sums[:LANES], sums[LANES:])


def step_of(u):
    return 2 * ((u % Z) % 2) + (u % Z) // 2


def main_kernel(
    order, v_hbm, coef_hbm, tab_hbm, early, late, v, coef, x, fs, fb, tab, sf, s, b, c, r,
    load_sem, tab_sem, plane_send, plane_recv, send, recv,
):
    grp = lax.axis_index("grp")
    dev = lax.axis_index("dev")
    z = (dev // 8) % 4
    mine = (dev // 32) * 8 + dev % 8
    here = grp * Z + z

    def at_plane(n):
        place = mine ^ n
        return place, (grp, (place // 8) * 32 + z * 8 + place % 8)

    def at_ring(height):
        height = lax.rem(height, G * Z)
        return (height // Z, (dev // 32) * 32 + (height % Z) * 8 + dev % 8)

    width = WORDS // SPLIT
    loads = [pltpu.make_async_copy(coef_hbm, coef, load_sem.at[0])]
    for part in range(SPLIT):
        for i in range(I):
            span = pl.ds(i * WORDS + part * width, width)
            n = 1 + part * I + i
            loads.append(pltpu.make_async_copy(v_hbm.at[:, span], v.at[:, span], load_sem.at[n]))
    for load in loads:
        load.start()

    barrier = pltpu.get_barrier_semaphore()

    def greet_plane(n, carry):
        _, device = at_plane(n)
        pl.semaphore_signal(barrier, inc=1, device_id=device, device_id_type=MESH)
        return carry

    def greet_ring(n, carry):
        pl.semaphore_signal(barrier, inc=1, device_id=at_ring(here + n), device_id_type=MESH)
        return carry

    lax.fori_loop(1, PLANE, greet_plane, 0)
    lax.fori_loop(1, G * Z, greet_ring, 0)

    def unpack(tile, carry):
        at = pl.multiple_of(tile * LANES, LANES)
        words = jnp.concatenate([v[:, pl.ds(at, LANES)], v[:, pl.ds(at + WORDS, LANES)]], axis=0)
        for byte in range(4):
            raw = jnp.bitwise_and(jnp.right_shift(words, 8 * byte), 255) - 128
            x[byte * TILES + tile] = raw.astype(F32)
        return carry

    def table_copy(u):
        t = (z + step_of(u)) % Z
        return pltpu.make_async_copy(tab_hbm.at[t, u // Z], tab.at[u], tab_sem.at[u])

    for part in range(SPLIT):
        for i in range(I):
            loads[1 + part * I + i].wait()
        if part == SPLIT - 1:
            for u in range(UNITS):
                table_copy(u).start()
        tiles = TILES // SPLIT
        lax.fori_loop(part * tiles, (part + 1) * tiles, unpack, 0, unroll=2)
    loads[0].wait()

    def fir(nb, carry):
        taps = [coef[pl.ds(nb * TAPS + k, 1), :] for k in range(TAPS)]
        window = [x[k * NB + nb] for k in range(TAPS - 1)]
        for f in range(F):
            window.append(x[(f + TAPS - 1) * NB + nb])
            total = window[0] * taps[0]
            for k in range(1, TAPS):
                total = total + window[k] * taps[k]
            window.pop(0)
            fs[pl.ds(f, 8, stride=STEP), :] = total
        at = pl.ds(pl.multiple_of(nb * LANES, LANES), LANES)
        for row in range(I * LOCAL):
            fb[row * F : (row + 1) * F, at] = fs[row * STEP : row * STEP + F, :].astype(BF16)
        return carry

    lax.fori_loop(0, NB, fir, 0)
    pl.semaphore_wait(barrier, PLANE + G * Z - 2)

    rows = C // UNITS
    low = lax.broadcasted_iota(jnp.int32, (rows, LANES), 1) < F

    def make(u, carry):
        table_copy(u).wait()
        spectra = lax.dot_general(
            tab[u], fb[...], (((1,), (1,)), ((), ())), preferred_element_type=F32
        )
        for i in range(I):
            for pair in range(LOCAL // 2):
                tile = (i * LOCAL // 2 + pair) * LANES
                re = spectra[:rows, tile : tile + LANES]
                im = spectra[rows:, tile : tile + LANES]
                even = jnp.where(low, re, pltpu.roll(im, F, 1))
                odd = jnp.where(low, pltpu.roll(re, F, 1), im)
                sf[i, pl.ds(2 * pair, rows, stride=LOCAL), :] = even
                sf[i, pl.ds(2 * pair + 1, rows, stride=LOCAL), :] = odd
            s[u, :, i] = sf[i].reshape(PLANE, PIECE, LANES).astype(BF16)

        def spread(n, carry):
            place, device = at_plane(n)
            pltpu.make_async_remote_copy(
                s.at[u, place], b.at[u, mine], plane_send.at[u], plane_recv.at[u], device, MESH
            ).start()
            return carry

        lax.fori_loop(1, PLANE, spread, 0)
        b[u, mine] = s[u, mine]
        return carry

    row = lax.broadcasted_iota(jnp.int32, (256, 256), 0)
    col = lax.broadcasted_iota(jnp.int32, (256, 256), 1)
    source = (row // 128) * 128 + ((row // 4) % 8) * 16 + ((row // 32) % 4) * 4 + row % 4
    swap = (source == col).astype(F32).astype(BF16)

    halves = (r, late)

    def ring_copy(half, u, other):
        to = lax.rem(grp + other, G)
        step = step_of(u)
        return pltpu.make_async_remote_copy(
            c.at[u],
            halves[half].at[grp, :, :, :, z],
            send.at[u, other],
            recv.at[u, other],
            at_ring(to * Z + (z + step) % Z),
            MESH,
        )

    def pass_on(half, u):
        whole = pl.ds(0, PLANE - 1)
        pltpu.make_async_copy(b.at[u, whole], b.at[u, whole], plane_recv.at[u]).wait()
        for pair in range(X // 2):
            pieces = [
                b[u, pair * 16 : pair * 16 + 16, i].reshape(256, LANES) for i in range(I)
            ]
            mixed = jnp.dot(swap, jnp.concatenate(pieces, axis=1), preferred_element_type=F32)
            for i in range(I):
                part = mixed[:, i * LANES : (i + 1) * LANES].astype(BF16)
                part = part.reshape(2, HC, ROWS, LANES)
                for n in range(2):
                    c[u, i, :, pair * 2 + n] = part[n]
        ring_copy(half, u, 1).start()

        @pl.when(u % Z == 0)
        def _():
            halves[half][grp, :, :, :, z] = c[u]

        @pl.when(u % Z != 0)
        def _():
            ring_copy(half, u, 0).start()

    lax.fori_loop(0, Z, make, 0)

    def both(u, carry):
        pass_on(0, u)
        return make(u + Z, carry)

    lax.fori_loop(0, Z, both, 0)

    def rest(u, carry):
        pass_on(1, u)
        return carry

    lax.fori_loop(Z, UNITS, rest, 0)

    def arrive(half):
        def one(u, carry):
            ring_copy(half, u, 1).wait_recv()

            @pl.when(u % Z != 0)
            def _():
                ring_copy(half, u, 0).wait_recv()

            return carry

        lax.fori_loop(half * Z, half * Z + Z, one, 0)

    arrive(0)

    def early_slot(n, carry):
        def block(g, i, ch, p):
            return r[g, i, ch, p].reshape(LANES, LANES)

        def store(i, ch, re, im):
            early[n, i, 0, ch] = re
            early[n, i, 1, ch] = im

        correlate(order, grp * SLOTS + n, block, store)
        return carry

    lax.fori_loop(0, SLOTS, early_slot, 0)
    arrive(1)

    def sent(u, carry):
        ring_copy(0, u, 1).wait_send()

        @pl.when(u % Z != 0)
        def _():
            ring_copy(0, u, 0).wait_send()

        whole = pl.ds(0, PLANE - 1)
        pltpu.make_async_copy(s.at[u, whole], s.at[u, whole], plane_send.at[u]).wait()
        return carry

    lax.fori_loop(0, UNITS, sent, 0)


def main(block_order, voltages):
    coef = jnp.asarray(prototype())
    table = jnp.asarray(dft_table())
    hbm = pl.BlockSpec(memory_space=pltpu.HBM)
    return pl.pallas_call(
        main_kernel,
        name="main",
        out_shape=(
            pltpu.VMEM((SLOTS, I, 2, HC, LANES, LANES), F32),
            pltpu.VMEM((G, I, HC, X, Z, ROWS, LANES), BF16),
        ),
        in_specs=[pl.BlockSpec(memory_space=pltpu.SMEM), hbm, hbm, hbm],
        out_specs=(pl.BlockSpec(memory_space=pltpu.VMEM), pl.BlockSpec(memory_space=pltpu.VMEM)),
        scratch_shapes=[
            pltpu.VMEM((LOCAL, I * WORDS), jnp.int32),
            pltpu.VMEM((NB * TAPS, LANES), F32),
            pltpu.VMEM((4 * TILES, I * LOCAL, LANES), F32),
            pltpu.VMEM((I * LOCAL * STEP, LANES), F32),
            pltpu.VMEM((I * LOCAL * F, N), BF16),
            pltpu.VMEM((UNITS, 2 * C // UNITS, N), BF16),
            pltpu.VMEM((I, C // UNITS * LOCAL, LANES), F32),
            pltpu.VMEM((UNITS, PLANE, I, PIECE, LANES), BF16),
            pltpu.VMEM((UNITS, PLANE, I, PIECE, LANES), BF16),
            pltpu.VMEM((UNITS, I, HC, X, ROWS, LANES), BF16),
            pltpu.VMEM((G, I, HC, X, Z, ROWS, LANES), BF16),
            pltpu.SemaphoreType.DMA((1 + SPLIT * I,)),
            pltpu.SemaphoreType.DMA((UNITS,)),
            pltpu.SemaphoreType.DMA((UNITS,)),
            pltpu.SemaphoreType.DMA((UNITS,)),
            pltpu.SemaphoreType.DMA((UNITS, G)),
            pltpu.SemaphoreType.DMA((UNITS, G)),
        ],
        compiler_params=pltpu.CompilerParams(
            collective_id=0, has_side_effects=True, vmem_limit_bytes=48 * 1024 * 1024
        ),
    )(block_order, voltages, coef, table)


def last_kernel(order, early, late, out, results, early_sem, sems):
    first = pltpu.make_async_copy(early, out.at[:, :, :, pl.ds(0, HC)], early_sem)
    first.start()
    grp = lax.axis_index("grp")

    def result(n):
        return pltpu.make_async_copy(results.at[n], out.at[n, :, :, pl.ds(HC, HC)], sems.at[n])

    def slot(n, carry):
        def block(g, i, ch, p):
            return late[g, i, ch, p].reshape(LANES, LANES)

        def store(i, ch, re, im):
            results[n, i, 0, ch] = re
            results[n, i, 1, ch] = im

        correlate(order, grp * SLOTS + n, block, store)
        result(n).start()
        return carry

    lax.fori_loop(0, SLOTS, slot, 0)
    first.wait()
    for n in range(SLOTS):
        result(n).wait()


def last(block_order, early, late):
    vmem = pl.BlockSpec(memory_space=pltpu.VMEM)
    return pl.pallas_call(
        last_kernel,
        name="last",
        out_shape=jax.ShapeDtypeStruct((SLOTS, I, 2, CH, LANES, LANES), F32),
        in_specs=[pl.BlockSpec(memory_space=pltpu.SMEM), vmem, vmem],
        out_specs=pl.BlockSpec(memory_space=pltpu.HBM),
        scratch_shapes=[
            pltpu.VMEM((SLOTS, I, 2, HC, LANES, LANES), F32),
            pltpu.SemaphoreType.DMA,
            pltpu.SemaphoreType.DMA((SLOTS,)),
        ],
        compiler_params=pltpu.CompilerParams(vmem_limit_bytes=24 * 1024 * 1024),
    )(block_order, early, late)


def on_device(voltages, block_order):
    early, late = main(block_order, voltages)
    return last(block_order, early, late)


def solution(mesh):
    in_specs = (P("dev", "grp"), P())
    out_specs = P("grp", None, None, "dev", None, None)
    return jax.shard_map(
        on_device, mesh=mesh, in_specs=in_specs, out_specs=out_specs, check_vma=False
    )
```

```python
import jax
import jax.numpy as jnp
import ml_dtypes
import numpy as np
from jax import lax
from jax.experimental import pallas as pl
from jax.experimental.pallas import tpu as pltpu
from jax.sharding import PartitionSpec as P

MESH = pl.DeviceIdType.MESH
BF16 = jnp.bfloat16
F32 = jnp.float32

A = 512
C = 1024
N = 2 * C
TAPS = 4
F = 64
I = 2
G = 2
LANES = 128
NB = N // LANES
LOCAL = 4
CH = 8
X = Z = Y = 4
PLANE = X * Y * 2
Q = 4
QC = CH // Q
PIECE = QC * I * LOCAL
EARLY = (Q - 1) * QC
ROWS = 8 * LOCAL
UNITS = Q * Z
STEP = F + 8
SPLIT = 2
WORDS = 34304
TILES = WORDS // LANES
SLOTS = 5


def prototype():
    position = np.arange(TAPS * N) + 0.5
    window = 0.5 - 0.5 * np.cos(2.0 * np.pi * position / (N * TAPS))
    coeffs = (np.sinc(position / N - TAPS / 2.0) * window).astype(np.float32) / 64
    return coeffs.reshape(TAPS, NB, LANES).transpose(1, 0, 2).reshape(NB * TAPS, LANES)


def dft_table():
    index = (np.arange(C)[:, None] * np.arange(N)[None, :]) % N
    angle = 2.0 * np.pi / N * np.arange(N)
    factor = N**-0.5
    parts = np.stack([np.cos(angle) * factor, -np.sin(angle) * factor])
    parts = parts.astype(np.float32).astype(ml_dtypes.bfloat16)[:, index]
    parts = parts.reshape(2, X, Z, 8, Q, QC, N).transpose(2, 4, 0, 1, 3, 5, 6)
    return np.ascontiguousarray(parts.reshape(Z, Q, 2 * C // UNITS, N))


def correlate(order, slot, block, store):
    entry = order[slot]
    one = lambda bound: (entry >= bound).astype(jnp.int32)
    p = one(4) + one(7) + one(9)
    q = entry - (3 * one(4) + 2 * one(7) + one(9))
    for i in range(I):
        for ch in range(QC):
            left, twisted, right = [], [], []
            for g in range(G):
                data = block(g, i, ch, p)
                wide = data.astype(F32)
                left.append(data)
                twisted.append(jnp.concatenate([wide[:, F:], -wide[:, :F]], axis=1).astype(BF16))
                right.append(block(g, i, ch, q))
            both = jnp.concatenate(
                [jnp.concatenate(left, axis=1), jnp.concatenate(twisted, axis=1)], axis=0
            )
            sums = lax.dot_general(
                both,
                jnp.concatenate(right, axis=1),
                (((1,), (1,)), ((), ())),
                preferred_element_type=F32,
            )
            sums = sums * (1.0 / (G * F))
            store(i, ch, sums[:LANES], sums[LANES:])


def step_of(u):
    return 2 * ((u % Z) % 2) + (u % Z) // 2


def main_kernel(
    order, v_hbm, coef_hbm, tab_hbm, early, late, v, coef, x, fs, fb, tab, sf, s, b, c, r0, r1, r2,
    ring_in, plane_in, load_sem, tab_sem, plane_send, plane_recv, send, recv,
):
    grp = lax.axis_index("grp")
    dev = lax.axis_index("dev")
    z = (dev // 8) % 4
    mine = (dev // 32) * 8 + dev % 8
    here = grp * Z + z

    def at_plane(n):
        place = mine ^ n
        return place, (grp, (place // 8) * 32 + z * 8 + place % 8)

    def at_ring(height):
        height = lax.rem(height, G * Z)
        return (height // Z, (dev // 32) * 32 + (height % Z) * 8 + dev % 8)

    width = WORDS // SPLIT
    loads = [pltpu.make_async_copy(coef_hbm, coef, load_sem.at[0])]
    for part in range(SPLIT):
        for i in range(I):
            span = pl.ds(i * WORDS + part * width, width)
            n = 1 + part * I + i
            loads.append(pltpu.make_async_copy(v_hbm.at[:, span], v.at[:, span], load_sem.at[n]))
    for load in loads:
        load.start()

    barrier = pltpu.get_barrier_semaphore()

    def greet_plane(n, carry):
        _, device = at_plane(n)
        pl.semaphore_signal(barrier, inc=1, device_id=device, device_id_type=MESH)
        return carry

    def greet_ring(n, carry):
        pl.semaphore_signal(barrier, inc=1, device_id=at_ring(here + n), device_id_type=MESH)
        return carry

    lax.fori_loop(1, PLANE, greet_plane, 0)
    lax.fori_loop(1, G * Z, greet_ring, 0)

    def unpack(tile, carry):
        at = pl.multiple_of(tile * LANES, LANES)
        words = jnp.concatenate([v[:, pl.ds(at, LANES)], v[:, pl.ds(at + WORDS, LANES)]], axis=0)
        for byte in range(4):
            raw = jnp.bitwise_and(jnp.right_shift(words, 8 * byte), 255) - 128
            x[byte * TILES + tile] = raw.astype(F32)
        return carry

    def table_copy(u):
        t = (z + step_of(u)) % Z
        return pltpu.make_async_copy(tab_hbm.at[t, u // Z], tab.at[u], tab_sem.at[u])

    for part in range(SPLIT):
        for i in range(I):
            loads[1 + part * I + i].wait()
        if part == SPLIT - 1:
            for u in range(UNITS):
                table_copy(u).start()
        tiles = TILES // SPLIT
        lax.fori_loop(part * tiles, (part + 1) * tiles, unpack, 0, unroll=2)
    loads[0].wait()

    def fir(nb, carry):
        taps = [coef[pl.ds(nb * TAPS + k, 1), :] for k in range(TAPS)]
        window = [x[k * NB + nb] for k in range(TAPS - 1)]
        for f in range(F):
            window.append(x[(f + TAPS - 1) * NB + nb])
            total = window[0] * taps[0]
            for k in range(1, TAPS):
                total = total + window[k] * taps[k]
            window.pop(0)
            fs[pl.ds(f, 8, stride=STEP), :] = total
        at = pl.ds(pl.multiple_of(nb * LANES, LANES), LANES)
        for row in range(I * LOCAL):
            fb[row * F : (row + 1) * F, at] = fs[row * STEP : row * STEP + F, :].astype(BF16)
        return carry

    lax.fori_loop(0, NB, fir, 0)
    pl.semaphore_wait(barrier, PLANE + G * Z - 2)

    rows = C // UNITS
    low = lax.broadcasted_iota(jnp.int32, (rows, LANES), 1) < F

    def make(u):
        table_copy(u).wait()
        spectra = lax.dot_general(
            tab[u], fb[...], (((1,), (1,)), ((), ())), preferred_element_type=F32
        )
        for i in range(I):
            for pair in range(LOCAL // 2):
                tile = (i * LOCAL // 2 + pair) * LANES
                re = spectra[:rows, tile : tile + LANES]
                im = spectra[rows:, tile : tile + LANES]
                even = jnp.where(low, re, pltpu.roll(im, F, 1))
                odd = jnp.where(low, pltpu.roll(re, F, 1), im)
                at = i * LOCAL + 2 * pair
                sf[pl.ds(at, rows, stride=I * LOCAL), :] = even
                sf[pl.ds(at + 1, rows, stride=I * LOCAL), :] = odd
        s[u] = sf[...].reshape(PLANE, PIECE, LANES).astype(BF16)

    def spread(u, source, landing):
        def one(n, carry):
            place, device = at_plane(n)
            pltpu.make_async_remote_copy(
                source.at[place], landing.at[mine], plane_send.at[u], plane_recv.at[u], device, MESH
            ).start()
            return carry

        lax.fori_loop(1, PLANE, one, 0)
        landing[mine] = source[mine]

    def gathered(u, landing):
        part = landing.at[pl.ds(0, PLANE - 1)]
        pltpu.make_async_copy(part, part, plane_recv.at[u]).wait()

    def ring_copy(quarter, u, other):
        source = c.at[u - Z] if quarter else s.at[u]
        landing = (r0, r1, r2, late)[quarter].at[grp, :, :, :, z] if quarter else ring_in.at[:, here]
        to = lax.rem(grp + other, G)
        return pltpu.make_async_remote_copy(
            source,
            landing,
            send.at[u, other],
            recv.at[u, other],
            at_ring(to * Z + (z + step_of(u)) % Z),
            MESH,
        )

    def ring_send(quarter, u, keep):
        ring_copy(quarter, u, 1).start()
        pl.when(u % Z == 0)(keep)

        @pl.when(u % Z != 0)
        def _():
            ring_copy(quarter, u, 0).start()

    def ring_wait(quarter, what):
        def one(u, carry):
            getattr(ring_copy(quarter, u, 1), what)()

            @pl.when(u % Z != 0)
            def _():
                getattr(ring_copy(quarter, u, 0), what)()

            return carry

        lax.fori_loop(quarter * Z, quarter * Z + Z, one, 0)

    row = lax.broadcasted_iota(jnp.int32, (256, 256), 0)
    col = lax.broadcasted_iota(jnp.int32, (256, 256), 1)
    source = (row // 128) * 128 + ((row // 4) % 8) * 16 + ((row // 32) % 2) * 8 + ((row // 64) % 2) * 4 + row % 4
    swap = (source == col).astype(F32).astype(BF16)

    def interleave(block, store):
        pieces = [block(xs).reshape(128, LANES) for xs in range(X)]
        wide = jnp.concatenate(
            [jnp.concatenate(pieces[:2], axis=0), jnp.concatenate(pieces[2:], axis=0)], axis=1
        )
        mixed = jnp.dot(swap, wide, preferred_element_type=F32)
        for xs in range(X):
            at, lane = xs % 2 * 128, xs // 2 * LANES
            part = mixed[at : at + 128, lane : lane + LANES].astype(BF16)
            store(xs, part.reshape(I, QC, ROWS, LANES))

    def first(u, carry):
        make(u)

        def keep():
            ring_in[:, here] = s[u]

        ring_send(0, u, keep)
        return carry

    def start(u, carry):
        make(u)
        spread(u, s.at[u], b.at[u - Z])
        return carry

    def pass_on(quarter, u):
        gathered(u, b.at[u - Z])

        def store(xs, part):
            c[u - Z, :, :, xs] = part

        interleave(lambda xs: b[u - Z, xs * 8 : xs * 8 + 8], store)

        def keep():
            (r0, r1, r2, late)[quarter][grp, :, :, :, z] = c[u - Z]

        ring_send(quarter, u, keep)

    lax.fori_loop(0, Z, first, 0)
    lax.fori_loop(Z, 2 * Z, start, 0)
    for quarter in range(1, Q - 1):

        def both(u, carry, quarter=quarter):
            pass_on(quarter, u)
            return start(u + Z, carry)

        lax.fori_loop(quarter * Z, quarter * Z + Z, both, 0)

    ring_wait(0, "wait_recv")
    spread(0, ring_in, plane_in)

    def rest(u, carry):
        pass_on(Q - 1, u)
        return carry

    lax.fori_loop(UNITS - Z, UNITS, rest, 0)

    gathered(0, plane_in)

    def turn(n, carry):
        def store(xs, part):
            r0[n // Z, :, :, xs, n % Z] = part

        interleave(lambda xs: plane_in[xs * 8 : xs * 8 + 8, n], store)
        return carry

    lax.fori_loop(0, G * Z, turn, 0)

    def sums(quarter, r):
        def one(n, carry):
            def block(g, i, ch, p):
                return r[g, i, ch, p].reshape(LANES, LANES)

            def store(i, ch, re, im):
                early[n, i, 0, quarter * QC + ch] = re
                early[n, i, 1, quarter * QC + ch] = im

            correlate(order, grp * SLOTS + n, block, store)
            return carry

        lax.fori_loop(0, SLOTS, one, 0)

    sums(0, r0)
    ring_wait(1, "wait_recv")
    sums(1, r1)
    ring_wait(2, "wait_recv")
    sums(2, r2)
    for quarter in range(Q):
        ring_wait(quarter, "wait_send")
    part = ring_in.at[pl.ds(0, PLANE - 1)]
    pltpu.make_async_copy(part, part, plane_send.at[0]).wait()

    def sent(u, carry):
        part = s.at[u, pl.ds(0, PLANE - 1)]
        pltpu.make_async_copy(part, part, plane_send.at[u]).wait()
        return carry

    lax.fori_loop(Z, UNITS, sent, 0)
    ring_wait(Q - 1, "wait_recv")


def main(block_order, voltages):
    coef = jnp.asarray(prototype())
    table = jnp.asarray(dft_table())
    hbm = pl.BlockSpec(memory_space=pltpu.HBM)
    return pl.pallas_call(
        main_kernel,
        name="main",
        out_shape=(
            pltpu.VMEM((SLOTS, I, 2, EARLY, LANES, LANES), F32),
            pltpu.VMEM((G, I, QC, X, Z, ROWS, LANES), BF16),
        ),
        in_specs=[pl.BlockSpec(memory_space=pltpu.SMEM), hbm, hbm, hbm],
        out_specs=(pl.BlockSpec(memory_space=pltpu.VMEM), pl.BlockSpec(memory_space=pltpu.VMEM)),
        scratch_shapes=[
            pltpu.VMEM((LOCAL, I * WORDS), jnp.int32),
            pltpu.VMEM((NB * TAPS, LANES), F32),
            pltpu.VMEM((4 * TILES, I * LOCAL, LANES), F32),
            pltpu.VMEM((I * LOCAL * STEP, LANES), F32),
            pltpu.VMEM((I * LOCAL * F, N), BF16),
            pltpu.VMEM((UNITS, 2 * C // UNITS, N), BF16),
            pltpu.VMEM((C // UNITS * I * LOCAL, LANES), F32),
            pltpu.VMEM((UNITS, PLANE, PIECE, LANES), BF16),
            pltpu.VMEM((UNITS - Z, PLANE, PIECE, LANES), BF16),
            pltpu.VMEM((UNITS - Z, I, QC, X, ROWS, LANES), BF16),
            pltpu.VMEM((G, I, QC, X, Z, ROWS, LANES), BF16),
            pltpu.VMEM((G, I, QC, X, Z, ROWS, LANES), BF16),
            pltpu.VMEM((G, I, QC, X, Z, ROWS, LANES), BF16),
            pltpu.VMEM((PLANE, G * Z, PIECE, LANES), BF16),
            pltpu.VMEM((PLANE, G * Z, PIECE, LANES), BF16),
            pltpu.SemaphoreType.DMA((1 + SPLIT * I,)),
            pltpu.SemaphoreType.DMA((UNITS,)),
            pltpu.SemaphoreType.DMA((UNITS,)),
            pltpu.SemaphoreType.DMA((UNITS,)),
            pltpu.SemaphoreType.DMA((UNITS, G)),
            pltpu.SemaphoreType.DMA((UNITS, G)),
        ],
        compiler_params=pltpu.CompilerParams(
            collective_id=0, has_side_effects=True, vmem_limit_bytes=48 * 1024 * 1024
        ),
    )(block_order, voltages, coef, table)


def last_kernel(order, early, late, out, results, early_sem, sems):
    first = pltpu.make_async_copy(early, out.at[:, :, :, pl.ds(0, EARLY)], early_sem)
    first.start()
    grp = lax.axis_index("grp")

    def result(n):
        return pltpu.make_async_copy(results.at[n], out.at[n, :, :, pl.ds(EARLY, QC)], sems.at[n])

    def slot(n, carry):
        def block(g, i, ch, p):
            return late[g, i, ch, p].reshape(LANES, LANES)

        def store(i, ch, re, im):
            results[n, i, 0, ch] = re
            results[n, i, 1, ch] = im

        correlate(order, grp * SLOTS + n, block, store)
        result(n).start()
        return carry

    lax.fori_loop(0, SLOTS, slot, 0)
    first.wait()
    for n in range(SLOTS):
        result(n).wait()


def last(block_order, early, late):
    vmem = pl.BlockSpec(memory_space=pltpu.VMEM)
    return pl.pallas_call(
        last_kernel,
        name="last",
        out_shape=jax.ShapeDtypeStruct((SLOTS, I, 2, CH, LANES, LANES), F32),
        in_specs=[pl.BlockSpec(memory_space=pltpu.SMEM), vmem, vmem],
        out_specs=pl.BlockSpec(memory_space=pltpu.HBM),
        scratch_shapes=[
            pltpu.VMEM((SLOTS, I, 2, QC, LANES, LANES), F32),
            pltpu.SemaphoreType.DMA,
            pltpu.SemaphoreType.DMA((SLOTS,)),
        ],
        compiler_params=pltpu.CompilerParams(vmem_limit_bytes=24 * 1024 * 1024),
    )(block_order, early, late)


def on_device(voltages, block_order):
    early, late = main(block_order, voltages)
    return last(block_order, early, late)


def solution(mesh):
    in_specs = (P("dev", "grp"), P())
    out_specs = P("grp", None, None, "dev", None, None)
    return jax.shard_map(
        on_device, mesh=mesh, in_specs=in_specs, out_specs=out_specs, check_vma=False
    )
```

```python
import jax
import jax.numpy as jnp
import ml_dtypes
import numpy as np
from jax import lax
from jax.experimental import pallas as pl
from jax.experimental.pallas import tpu as pltpu
from jax.sharding import PartitionSpec as P

MESH = pl.DeviceIdType.MESH
BF16 = jnp.bfloat16
F32 = jnp.float32

A = 512
C = 1024
N = 2 * C
TAPS = 4
F = 64
I = 2
G = 2
LANES = 128
NB = N // LANES
LOCAL = 4
CH = 8
X = Z = Y = 4
PLANE = X * Y * 2
Q = 4
QC = CH // Q
PIECE = QC * I * LOCAL
EARLY = (Q - 1) * QC
ROWS = 8 * LOCAL
UNITS = Q * Z
SPLIT = 4
WORDS = 34304
TILES = WORDS // LANES
SLOTS = 5


def prototype():
    position = np.arange(TAPS * N) + 0.5
    window = 0.5 - 0.5 * np.cos(2.0 * np.pi * position / (N * TAPS))
    coeffs = (np.sinc(position / N - TAPS / 2.0) * window).astype(np.float32) / 64
    return coeffs.reshape(TAPS, NB, LANES).transpose(1, 0, 2).reshape(NB * TAPS, LANES)


def dft_table():
    index = (np.arange(C)[:, None] * np.arange(N)[None, :]) % N
    angle = 2.0 * np.pi / N * np.arange(N)
    factor = N**-0.5
    parts = np.stack([np.cos(angle) * factor, -np.sin(angle) * factor])
    parts = parts.astype(np.float32).astype(ml_dtypes.bfloat16)[:, index]
    parts = parts.reshape(2, X, Z, 8, Q, QC, N).transpose(2, 4, 0, 1, 3, 5, 6)
    return np.ascontiguousarray(parts.reshape(Z, Q, 2 * C // UNITS, N))


def correlate(order, slot, block, store):
    entry = order[slot]
    one = lambda bound: (entry >= bound).astype(jnp.int32)
    p = one(4) + one(7) + one(9)
    q = entry - (3 * one(4) + 2 * one(7) + one(9))
    for i in range(I):
        for ch in range(QC):
            left, twisted, right = [], [], []
            for g in range(G):
                data = block(g, i, ch, p)
                wide = data.astype(F32)
                left.append(data)
                twisted.append(jnp.concatenate([wide[:, F:], -wide[:, :F]], axis=1).astype(BF16))
                right.append(block(g, i, ch, q))
            both = jnp.concatenate(
                [jnp.concatenate(left, axis=1), jnp.concatenate(twisted, axis=1)], axis=0
            )
            sums = lax.dot_general(
                both,
                jnp.concatenate(right, axis=1),
                (((1,), (1,)), ((), ())),
                preferred_element_type=F32,
            )
            sums = sums * (1.0 / (G * F))
            store(i, ch, sums[:LANES], sums[LANES:])


def step_of(u):
    n = u % Z
    return n + n // 2 - 2 * (n // 3)


def main_kernel(
    order_hbm, v_hbm, coef_hbm, tab_hbm, early, late, order, v, coef, x, fb, regroup, total, tab, sf, s, b, c, r0, r1, r2,
    ring_in, plane_in, order_sem, load_sem, tab_sem, plane_send, plane_recv, send, recv,
):
    grp = lax.axis_index("grp")
    dev = lax.axis_index("dev")
    z = (dev // 8) % 4
    mine = (dev // 32) * 8 + dev % 8
    here = grp * Z + z

    def at_plane(n):
        place = mine ^ n
        return place, (grp, (place // 8) * 32 + z * 8 + place % 8)

    def at_ring(height):
        height = lax.rem(height, G * Z)
        return (height // Z, (dev // 32) * 32 + (height % Z) * 8 + dev % 8)

    def table_copy(u):
        t = (z + step_of(u)) % Z
        return pltpu.make_async_copy(tab_hbm.at[t, u // Z], tab.at[u], tab_sem.at[u])

    width = WORDS // SPLIT
    loads = [pltpu.make_async_copy(coef_hbm, coef, load_sem.at[0])]
    for part in range(SPLIT):
        for i in range(I):
            span = pl.ds(i * WORDS + part * width, width)
            n = 1 + part * I + i
            loads.append(pltpu.make_async_copy(v_hbm.at[:, span], v.at[:, span], load_sem.at[n]))
    for load in loads:
        load.start()
    table_copy(0).start()
    slots = pltpu.make_async_copy(order_hbm, order, order_sem)
    slots.start()

    barrier = pltpu.get_barrier_semaphore()

    def greet_plane(n, carry):
        _, device = at_plane(n)
        pl.semaphore_signal(barrier, inc=1, device_id=device, device_id_type=MESH)
        return carry

    def greet_ring(n, carry):
        pl.semaphore_signal(barrier, inc=1, device_id=at_ring(here + n), device_id_type=MESH)
        return carry

    lax.fori_loop(1, PLANE, greet_plane, 0)
    lax.fori_loop(1, G * Z, greet_ring, 0)

    row = lax.broadcasted_iota(jnp.int32, regroup.shape, 0)
    col = lax.broadcasted_iota(jnp.int32, regroup.shape, 1)
    regroup[...] = ((col % F) * (I * LOCAL) + col // F == row).astype(F32).astype(BF16)

    def unpack(tile, carry):
        at = pl.multiple_of(tile * LANES, LANES)
        words = jnp.concatenate([v[:, pl.ds(at, LANES)], v[:, pl.ds(at + WORDS, LANES)]], axis=0)
        for byte in range(4):
            raw = jnp.bitwise_and(jnp.right_shift(words, 8 * byte), 255) - 128
            x[byte * TILES + tile] = raw.astype(F32)
        return carry

    for part in range(SPLIT):
        for i in range(I):
            loads[1 + part * I + i].wait()
        if part == SPLIT - 1:
            for u in range(1, UNITS):
                table_copy(u).start()
        tiles = TILES // SPLIT
        lax.fori_loop(part * tiles, (part + 1) * tiles, unpack, 0, unroll=2)
    loads[0].wait()

    def fir(nb):
        taps = [coef[pl.ds(nb * TAPS + k, 1), :] for k in range(TAPS)]
        window = [x[k * NB + nb] for k in range(TAPS - 1)]
        at = pl.ds(pl.multiple_of(nb * LANES, LANES), LANES)
        for f in range(0, F, 2):
            sums = []
            for n in range(2):
                window.append(x[(f + n + TAPS - 1) * NB + nb])
                one = window[0] * taps[0]
                for k in range(1, TAPS):
                    one = one + window[k] * taps[k]
                window.pop(0)
                sums.append(one)
            fb[f * 8 : f * 8 + 16, at] = jnp.concatenate(sums, axis=0).astype(BF16)

    def dft(table, frames):
        return lax.dot_general(
            table, frames, (((1,), (1,)), ((), ())), preferred_element_type=F32
        )

    def partial(n):
        at = pl.ds(pl.multiple_of(n * 2 * LANES, 2 * LANES), 2 * LANES)
        return dft(tab[0, :, at], fb[:, at])

    fir(0)
    fir(1)
    table_copy(0).wait()
    total[...] = jnp.zeros_like(total)

    def blocks(n, carry):
        total[...] += partial(n - 1)
        fir(2 * n)
        fir(2 * n + 1)
        return carry

    lax.fori_loop(1, NB // 2, blocks, 0)
    total[...] += partial(NB // 2 - 1)
    pl.semaphore_wait(barrier, PLANE + G * Z - 2)

    rows = C // UNITS
    low = lax.broadcasted_iota(jnp.int32, (rows, LANES), 1) < F

    def make(u):
        table_copy(u).wait()
        finish(u, dft(tab[u], fb[...]))

    def finish(u, spectra):
        spectra = jnp.dot(spectra.astype(BF16), regroup[...], preferred_element_type=F32)
        for i in range(I):
            for pair in range(LOCAL // 2):
                tile = (i * LOCAL // 2 + pair) * LANES
                re = spectra[:rows, tile : tile + LANES]
                im = spectra[rows:, tile : tile + LANES]
                even = jnp.where(low, re, pltpu.roll(im, F, 1))
                odd = jnp.where(low, pltpu.roll(re, F, 1), im)
                at = i * LOCAL + 2 * pair
                sf[pl.ds(at, rows, stride=I * LOCAL), :] = even
                sf[pl.ds(at + 1, rows, stride=I * LOCAL), :] = odd
        s[u] = sf[...].reshape(PLANE, PIECE, LANES).astype(BF16)

    def spread(u, source, landing):
        def one(n, carry):
            place, device = at_plane(n)
            pltpu.make_async_remote_copy(
                source.at[place], landing.at[mine], plane_send.at[u], plane_recv.at[u], device, MESH
            ).start()
            return carry

        lax.fori_loop(1, PLANE, one, 0)
        landing[mine] = source[mine]

    def gathered(u, landing):
        part = landing.at[pl.ds(0, PLANE - 1)]
        pltpu.make_async_copy(part, part, plane_recv.at[u]).wait()

    def ring_copy(quarter, u, other):
        source = c.at[u - Z] if quarter else s.at[u]
        landing = (r0, r1, r2, late)[quarter].at[grp, :, :, :, z] if quarter else ring_in.at[:, here]
        to = lax.rem(grp + other, G)
        return pltpu.make_async_remote_copy(
            source,
            landing,
            send.at[u, other],
            recv.at[u, other],
            at_ring(to * Z + (z + step_of(u)) % Z),
            MESH,
        )

    def ring_send(quarter, u, keep):
        ring_copy(quarter, u, 1).start()
        pl.when(u % Z == 0)(keep)

        @pl.when(u % Z != 0)
        def _():
            ring_copy(quarter, u, 0).start()

    def ring_wait(quarter, what):
        def one(u, carry):
            getattr(ring_copy(quarter, u, 1), what)()

            @pl.when(u % Z != 0)
            def _():
                getattr(ring_copy(quarter, u, 0), what)()

            return carry

        lax.fori_loop(quarter * Z, quarter * Z + Z, one, 0)

    row = lax.broadcasted_iota(jnp.int32, (256, 256), 0)
    col = lax.broadcasted_iota(jnp.int32, (256, 256), 1)
    source = (row // 128) * 128 + ((row // 4) % 8) * 16 + ((row // 32) % 2) * 8 + ((row // 64) % 2) * 4 + row % 4
    swap = (source == col).astype(F32).astype(BF16)

    def interleave(block, store):
        pieces = [block(xs).reshape(128, LANES) for xs in range(X)]
        wide = jnp.concatenate(
            [jnp.concatenate(pieces[:2], axis=0), jnp.concatenate(pieces[2:], axis=0)], axis=1
        )
        mixed = jnp.dot(swap, wide, preferred_element_type=F32)
        for xs in range(X):
            at, lane = xs % 2 * 128, xs // 2 * LANES
            part = mixed[at : at + 128, lane : lane + LANES].astype(BF16)
            store(xs, part.reshape(I, QC, ROWS, LANES))

    def ring_first(u):
        def keep():
            ring_in[:, here] = s[u]

        ring_send(0, u, keep)

    def first(u, carry):
        make(u)
        ring_first(u)
        return carry

    def start(u, carry):
        make(u)
        spread(u, s.at[u], b.at[u - Z])
        return carry

    def pass_on(quarter, u):
        gathered(u, b.at[u - Z])

        def store(xs, part):
            c[u - Z, :, :, xs] = part

        interleave(lambda xs: b[u - Z, xs * 8 : xs * 8 + 8], store)

        def keep():
            (r0, r1, r2, late)[quarter][grp, :, :, :, z] = c[u - Z]

        ring_send(quarter, u, keep)

    finish(0, total[...])
    ring_first(0)
    lax.fori_loop(1, Z, first, 0)
    lax.fori_loop(Z, 2 * Z, start, 0)
    for quarter in range(1, Q - 1):

        def both(u, carry, quarter=quarter):
            pass_on(quarter, u)
            return start(u + Z, carry)

        lax.fori_loop(quarter * Z, quarter * Z + Z, both, 0)

    ring_wait(0, "wait_recv")
    spread(0, ring_in, plane_in)

    def rest(u, carry):
        pass_on(Q - 1, u)
        return carry

    lax.fori_loop(UNITS - Z, UNITS, rest, 0)

    gathered(0, plane_in)

    def turn(n, carry):
        def store(xs, part):
            r0[n // Z, :, :, xs, n % Z] = part

        interleave(lambda xs: plane_in[xs * 8 : xs * 8 + 8, n], store)
        return carry

    lax.fori_loop(0, G * Z, turn, 0)

    def sums(quarter, r):
        def one(n, carry):
            def block(g, i, ch, p):
                return r[g, i, ch, p].reshape(LANES, LANES)

            def store(i, ch, re, im):
                early[n, i, 0, quarter * QC + ch] = re
                early[n, i, 1, quarter * QC + ch] = im

            correlate(order, grp * SLOTS + n, block, store)
            return carry

        lax.fori_loop(0, SLOTS, one, 0)

    slots.wait()
    sums(0, r0)
    ring_wait(1, "wait_recv")
    sums(1, r1)
    ring_wait(2, "wait_recv")
    sums(2, r2)
    for quarter in range(Q):
        ring_wait(quarter, "wait_send")
    part = ring_in.at[pl.ds(0, PLANE - 1)]
    pltpu.make_async_copy(part, part, plane_send.at[0]).wait()

    def sent(u, carry):
        part = s.at[u, pl.ds(0, PLANE - 1)]
        pltpu.make_async_copy(part, part, plane_send.at[u]).wait()
        return carry

    lax.fori_loop(Z, UNITS, sent, 0)
    ring_wait(Q - 1, "wait_recv")


def main(block_order, voltages):
    coef = jnp.asarray(prototype())
    table = jnp.asarray(dft_table())
    hbm = pl.BlockSpec(memory_space=pltpu.HBM)
    return pl.pallas_call(
        main_kernel,
        name="main",
        out_shape=(
            pltpu.VMEM((SLOTS, I, 2, EARLY, LANES, LANES), F32),
            pltpu.VMEM((G, I, QC, X, Z, ROWS, LANES), BF16),
        ),
        in_specs=[hbm, hbm, hbm, hbm],
        out_specs=(pl.BlockSpec(memory_space=pltpu.VMEM), pl.BlockSpec(memory_space=pltpu.VMEM)),
        scratch_shapes=[
            pltpu.SMEM((10,), jnp.int32),
            pltpu.VMEM((LOCAL, I * WORDS), jnp.int32),
            pltpu.VMEM((NB * TAPS, LANES), F32),
            pltpu.VMEM((4 * TILES, I * LOCAL, LANES), F32),
            pltpu.VMEM((I * LOCAL * F, N), BF16),
            pltpu.VMEM((I * LOCAL * F, I * LOCAL * F), BF16),
            pltpu.VMEM((2 * C // UNITS, I * LOCAL * F), F32),
            pltpu.VMEM((UNITS, 2 * C // UNITS, N), BF16),
            pltpu.VMEM((C // UNITS * I * LOCAL, LANES), F32),
            pltpu.VMEM((UNITS, PLANE, PIECE, LANES), BF16),
            pltpu.VMEM((UNITS - Z, PLANE, PIECE, LANES), BF16),
            pltpu.VMEM((UNITS - Z, I, QC, X, ROWS, LANES), BF16),
            pltpu.VMEM((G, I, QC, X, Z, ROWS, LANES), BF16),
            pltpu.VMEM((G, I, QC, X, Z, ROWS, LANES), BF16),
            pltpu.VMEM((G, I, QC, X, Z, ROWS, LANES), BF16),
            pltpu.VMEM((PLANE, G * Z, PIECE, LANES), BF16),
            pltpu.VMEM((PLANE, G * Z, PIECE, LANES), BF16),
            pltpu.SemaphoreType.DMA,
            pltpu.SemaphoreType.DMA((1 + SPLIT * I,)),
            pltpu.SemaphoreType.DMA((UNITS,)),
            pltpu.SemaphoreType.DMA((UNITS,)),
            pltpu.SemaphoreType.DMA((UNITS,)),
            pltpu.SemaphoreType.DMA((UNITS, G)),
            pltpu.SemaphoreType.DMA((UNITS, G)),
        ],
        compiler_params=pltpu.CompilerParams(
            collective_id=0, has_side_effects=True, vmem_limit_bytes=48 * 1024 * 1024
        ),
    )(block_order, voltages, coef, table)


def last_kernel(order_hbm, early, late, out, order, results, order_sem, early_sem, sems):
    slots = pltpu.make_async_copy(order_hbm, order, order_sem)
    slots.start()
    first = pltpu.make_async_copy(early, out.at[:, :, :, pl.ds(0, EARLY)], early_sem)
    first.start()
    grp = lax.axis_index("grp")

    def result(n):
        return pltpu.make_async_copy(results.at[n], out.at[n, :, :, pl.ds(EARLY, QC)], sems.at[n])

    def slot(n, carry):
        def block(g, i, ch, p):
            return late[g, i, ch, p].reshape(LANES, LANES)

        def store(i, ch, re, im):
            results[n, i, 0, ch] = re
            results[n, i, 1, ch] = im

        correlate(order, grp * SLOTS + n, block, store)
        result(n).start()
        return carry

    slots.wait()
    lax.fori_loop(0, SLOTS, slot, 0)
    first.wait()
    for n in range(SLOTS):
        result(n).wait()


def last(block_order, early, late):
    vmem = pl.BlockSpec(memory_space=pltpu.VMEM)
    return pl.pallas_call(
        last_kernel,
        name="last",
        out_shape=jax.ShapeDtypeStruct((SLOTS, I, 2, CH, LANES, LANES), F32),
        in_specs=[pl.BlockSpec(memory_space=pltpu.HBM), vmem, vmem],
        out_specs=pl.BlockSpec(memory_space=pltpu.HBM),
        scratch_shapes=[
            pltpu.SMEM((10,), jnp.int32),
            pltpu.VMEM((SLOTS, I, 2, QC, LANES, LANES), F32),
            pltpu.SemaphoreType.DMA,
            pltpu.SemaphoreType.DMA,
            pltpu.SemaphoreType.DMA((SLOTS,)),
        ],
        compiler_params=pltpu.CompilerParams(vmem_limit_bytes=24 * 1024 * 1024),
    )(block_order, early, late)


def on_device(voltages, block_order):
    early, late = main(block_order, voltages)
    return last(block_order, early, late)


def solution(mesh):
    in_specs = (P("dev", "grp"), P())
    out_specs = P("grp", None, None, "dev", None, None)
    return jax.shard_map(
        on_device, mesh=mesh, in_specs=in_specs, out_specs=out_specs, check_vma=False
    )
```
